32 devices in a mesh: row: 4 (over y, x), col: 8 (over z, core).
Axes of the slice: x: 2, y: 2, z: 4, core: 2. Of those that a mesh axis runs over, the one named last changes fastest.
Arguments:
- coarse_left: float32 [32, 16384], P('col', 'row'), may hold values from -3 to 3
- coarse_right: float32 [32, 16384], P('row', 'col'), may hold values from -3 to 3
- stencil_left: int32 [65536], P('row'), may hold values from -1 to 16384, as said below
- weights_left: float32 [4, 65536], P(None, 'row'), may hold values from 0.1 to 0.6
- stencil_right: int32 [65536], P('col'), may hold values from -1 to 16384, as said below
- weights_right: float32 [4, 65536], P(None, 'col'), may hold values from 0.1 to 0.6
- tile_mask: int32 [16, 16], P('row', 'col'), may hold values 0 or 1
- sample_rows: int32 [16, 16, 2048], P('row', 'col'), may hold values from 0 to 4095
- sample_cols: int32 [16, 16, 2048], P('row', 'col'), may hold values from 0 to 4095
- sample_values: float32 [16, 16, 2048], P('row', 'col'), may hold values from -6 to 6
Outputs:
- left_new: float32 [32, 65536], P('col', 'row')
- right_new: float32 [32, 65536], P('row', 'col')
The draws below stay inside these ranges and needn't reach their ends.
Inputs may be any that keep to these rules, and one draw needn't show every extreme that they name: stencil_left[i] is i // 4 - 1, i // 4 or i // 4 + 1. stencil_right[j] is j // 4 - 1, j // 4 or j // 4 + 1.
All inputs are finite; a program needn't handle non-finite values. No bound on the sum of `tile_mask` on one device may be relied on, other than what follows from the above.
Results may differ from the reference program's by a relative error of at most 0.0001.
Values sent between devices are 32-bit elements; how exact they have to be, the bound alone decides.
No kernel may reach another device: no remote copies, remote signals or barrier semaphores. Data moves between devices by JAX's collectives and lax.ppermute only.
A program may use at most 128 MiB of HBM per device.

```python
import jax
import jax.numpy as jnp
from jax import lax

NF = 65536
NC = 16384
RANK = 32
TAPS = 4
TILES = 16
TILE = 4096
SPT = 2048


def draw_stencil_left(key, part):
    noise = jax.random.randint(jax.random.fold_in(key, 11), (NF,), -1, 2, dtype=jnp.int32)
    return (jnp.arange(NF, dtype=jnp.int32) // 4 + noise).astype(jnp.int32)


def draw_stencil_right(key, part):
    noise = jax.random.randint(jax.random.fold_in(key, 23), (NF,), -1, 2, dtype=jnp.int32)
    return (jnp.arange(NF, dtype=jnp.int32) // 4 + noise).astype(jnp.int32)


def with_ends(result, rng, smallest, top_value):
    longest = result.shape.index(max(result.shape))
    spots = []
    for shift in (0, 1):
        where = [jax.random.randint(jax.random.fold_in(rng, axis), (), 0, length) for axis, length in enumerate(result.shape)]
        where[longest] = (where[longest] + shift) % result.shape[longest]
        spots.append(tuple(where))
    return result.at[spots[0]].set(smallest).at[spots[1]].set(top_value)


def block_scale(key, shape, cuts, low, largest):
    def one(axis_at, parts):
        heights = jax.random.uniform(jax.random.fold_in(jax.random.fold_in(key, 6), axis_at), (parts,), jnp.float32, low / len(cuts), largest / len(cuts))
        return jnp.repeat(jnp.exp(heights), shape[axis_at] // parts).reshape((-1,) + (1,) * (len(shape) - axis_at - 1))

    gain = one(*cuts[0])
    for cut in cuts[1:]:
        gain = gain * one(*cut)
    return gain


def bell_draw(stream_key, shape, deviation, reach, shards=(), kind=jnp.bfloat16):
    factor_of = block_scale(stream_key, shape, shards, -0.22, 0.18) if shards else 1.0
    array = jax.random.normal(stream_key, shape, jnp.float32) * deviation * factor_of
    return jnp.minimum(jnp.maximum(array, -reach), reach).astype(kind)


def setup_inputs(seed: int = 0) -> dict:
    key_of = jax.random.split(jax.random.key(seed), 11)
    return {
        "coarse_left": bell_draw(key_of[0], (RANK, NC), 0.5, 3.0, ((0, 8), (1, 4)), jnp.float32),
        "coarse_right": bell_draw(key_of[1], (RANK, NC), 0.5, 3.0, ((0, 4), (1, 8)), jnp.float32),
        "stencil_left": draw_stencil_left(jax.random.fold_in(key_of[10], 71), 0),
        "weights_left": jnp.clip(0.1 + 0.5 * jax.random.uniform(key_of[3], (TAPS, NF), jnp.float32) ** block_scale(key_of[3], (TAPS, NF), ((1, 4),), -0.2, 0.2), 0.1, 0.6),
        "stencil_right": draw_stencil_right(jax.random.fold_in(key_of[10], 71), 0),
        "weights_right": jnp.clip(0.1 + 0.5 * jax.random.uniform(key_of[5], (TAPS, NF), jnp.float32) ** block_scale(key_of[5], (TAPS, NF), ((1, 8),), -0.2, 0.2), 0.1, 0.6),
        "tile_mask": with_ends((jax.random.randint(key_of[6], (TILES, TILES), 0, 2) < 1).astype(jnp.int32), jax.random.fold_in(key_of[6], 1), 0, 1),
        "sample_rows": with_ends(jax.random.randint(key_of[7], (TILES, TILES, SPT), 0, TILE), jax.random.fold_in(key_of[7], 1), 0, TILE - 1).astype(jnp.int32),
        "sample_cols": with_ends(jax.random.randint(key_of[8], (TILES, TILES, SPT), 0, TILE), jax.random.fold_in(key_of[8], 1), 0, TILE - 1).astype(jnp.int32),
        "sample_values": bell_draw(key_of[9], (TILES, TILES, SPT), 1.0, 6.0, ((0, 4), (1, 8)), jnp.float32),
    }


def spread(padded, base, weights, offset):
    start_at = base - offset + 2
    columns_at = start_at[None, :] + jnp.arange(4, dtype=jnp.int32)[:, None]
    values = jnp.take(padded, columns_at, axis=1)
    return jnp.sum(values * weights[None], axis=1)


def reference(coarse_left, coarse_right, stencil_left, weights_left, stencil_right, weights_right, tile_mask, sample_rows, sample_cols, sample_values):
    fine_left = spread(jnp.pad(coarse_left, ((0, 0), (3, 3))), stencil_left, weights_left, 0)
    fine_right = spread(jnp.pad(coarse_right, ((0, 0), (3, 3))), stencil_right, weights_right, 0)
    starts = jnp.arange(TILES, dtype=jnp.int32) * TILE
    row_start = jnp.broadcast_to(starts[:, None], (TILES, TILES)).reshape(-1)
    col_start = jnp.broadcast_to(starts[None, :], (TILES, TILES)).reshape(-1)
    rows_all = (sample_rows.reshape(TILES * TILES, SPT) + row_start[:, None]).astype(jnp.int32)
    cols_all = (sample_cols.reshape(TILES * TILES, SPT) + col_start[:, None]).astype(jnp.int32)
    values_all = sample_values.reshape(TILES * TILES, SPT)
    keeping = jnp.broadcast_to(tile_mask.reshape(-1, 1).astype(jnp.float32), (TILES * TILES, SPT))
    width = min(SPT, 4096)
    pieces = TILES * TILES * SPT // width
    rows_all = rows_all.reshape(pieces, width)
    cols_all = cols_all.reshape(pieces, width)
    values_all = values_all.reshape(pieces, width)
    keeping = keeping.reshape(pieces, width)

    def visit(carry, block):
        grad_left, grad_right = carry
        rows_here, cols_here, values_here, keep_here = block
        left_cols = jnp.take(fine_left, rows_here, axis=1)
        right_cols = jnp.take(fine_right, cols_here, axis=1)
        error = keep_here * (jnp.sum(left_cols * right_cols, axis=0) - values_here)
        grad_left = grad_left.at[:, rows_here].add(error[None, :] * right_cols)
        grad_right = grad_right.at[:, cols_here].add(error[None, :] * left_cols)
        return (grad_left, grad_right), None

    empty = jnp.zeros((RANK, NF), jnp.float32)
    (grad_left, grad_right), _ = lax.scan(visit, (empty, empty), (rows_all, cols_all, values_all, keeping))
    step_size = 4.0 * TILE / (SPT * TILES)
    return fine_left - step_size * grad_left, fine_right - step_size * grad_right
```

```python
import functools

import jax
import jax.numpy as jnp
from jax import lax
from jax.experimental import pallas as pl
from jax.experimental.pallas import tpu as pltpu
from jax.sharding import PartitionSpec as P

TILES = 16
TILE = 4096
SPT = 2048
TAPS = 4
LOW = 2
HIGH = 3
CHUNK = 256
READ = 1024
ADD = 1024


def with_edges(block, axis):
    count = lax.axis_size(axis)
    width = block.shape[1]
    forward = [(i, i + 1) for i in range(count - 1)]
    backward = [(target, source) for source, target in forward]
    low = lax.ppermute(block[:, width - LOW :], axis, forward)
    high = lax.ppermute(block[:, :HIGH], axis, backward)
    filler = jnp.zeros((block.shape[0], 128 - LOW - HIGH), jnp.float32)
    return jnp.concatenate([low, block, high, filler], axis=1)


def split(values):
    high = values.astype(jnp.bfloat16)
    return high, (values - high.astype(jnp.float32)).astype(jnp.bfloat16)


def interpolate(padded, stencil, weights, table, out, first, last, offset, tile):
    rank = padded.shape[0]
    rows = lax.broadcasted_iota(jnp.int32, (rank, 128), 0)
    own = (rows >= first) & (rows < last)

    def group(g, _):
        column = pl.multiple_of(tile * TILE + g * 1024, 1024)
        start = pl.multiple_of(tile * (TILE // 4) + g * 256, 256)
        base = stencil[tile * (TILE // 1024) + g] - (offset + start - 1)
        window = padded[:, pl.ds(start, 384)]
        for u in range(8):
            low = 128 * (u // 4) + (64 if u % 4 == 3 else 0)
            part = window[:, low : low + 128]
            total = None
            for t in range(TAPS):
                at = jnp.broadcast_to(base[u : u + 1, :] + (t - low), (rank, 128))
                taken = jnp.take_along_axis(part, at, axis=1, mode="promise_in_bounds")
                term = taken * weights[t : t + 1, pl.ds(column + 128 * u, 128)]
                total = term if total is None else total + term
            high, rest = split(total)
            to = pl.ds(pl.multiple_of((g * 4 + u // 2) * rank, rank), rank)
            lane = (u % 2) * 128
            table[tile, to, lane : lane + 128] = high
            table[tile, to, CHUNK + lane : CHUNK + lane + 128] = rest
            out[:, pl.ds(column + 128 * u, 128)] = jnp.where(own, total, 0.0)
        return 0

    lax.fori_loop(0, TILE // 1024, group, 0)


def one_hot(index):
    lanes = lax.broadcasted_iota(jnp.int32, (CHUNK, index.shape[1]), 0)
    return jnp.where(lanes == (index & (CHUNK - 1)), 1.0, 0.0).astype(jnp.bfloat16)


def read(table, index, rank):
    hot = one_hot(index)
    found = jnp.dot(
        table, jnp.concatenate([hot, hot], axis=0), preferred_element_type=jnp.float32
    )
    chunk = jnp.broadcast_to(index >> 8, (rank, index.shape[1]))
    taken = found[:rank]
    for c in range(1, found.shape[0] // rank):
        taken = jnp.where(chunk == c, found[c * rank : (c + 1) * rank], taken)
    return taken


def add(out, values, index, tile):
    rank = values.shape[0]
    hot = one_hot(index)
    chunk = jnp.broadcast_to(index >> 8, values.shape)
    high, rest = split(values)
    zero = jnp.zeros(values.shape, jnp.bfloat16)
    left = jnp.concatenate(
        [
            jnp.concatenate(
                [jnp.where(chunk == c, high, zero), jnp.where(chunk == c, rest, zero)], axis=1
            )
            for c in range(TILE // CHUNK)
        ],
        axis=0,
    )
    summed = lax.dot_general(
        left,
        jnp.concatenate([hot, hot], axis=1),
        (((1,), (1,)), ((), ())),
        preferred_element_type=jnp.float32,
    )
    for c in range(TILE // CHUNK):
        at = pl.ds(pl.multiple_of(tile * TILE + c * CHUNK, CHUNK), CHUNK)
        out[:, at] += summed[c * rank : (c + 1) * rank]


def step(
    place,
    mask,
    left,
    right,
    stencil_left,
    weights_left,
    stencil_right,
    weights_right,
    rows,
    cols,
    values,
    left_out,
    right_out,
    left_table,
    right_table,
    *,
    eta,
):
    rank = left.shape[0]
    tile_rows, tile_cols, samples = rows.shape
    for a in range(tile_rows):
        interpolate(
            left, stencil_left, weights_left, left_table, left_out, place[0], place[1], place[2], a
        )
    for b in range(tile_cols):
        interpolate(
            right, stencil_right, weights_right, right_table, right_out, place[3], place[4], place[5], b
        )

    def visit(a, b):
        @pl.when(mask[a, b] != 0)
        def _():
            scale = mask[a, b].astype(jnp.float32) * (-eta)

            def batch(i, _):
                for_left, for_right, at_rows, at_cols = [], [], [], []
                for j in range(ADD // READ):
                    at = pl.ds(pl.multiple_of(i * ADD + j * READ, READ), READ)
                    row = rows[a, b : b + 1, at]
                    col = cols[a, b : b + 1, at]
                    left_cols = read(left_table[a], row, rank)
                    right_cols = read(right_table[b], col, rank)
                    product = jnp.sum(left_cols * right_cols, axis=0, keepdims=True)
                    error = scale * (product - values[a, b : b + 1, at])
                    for_left.append(error * right_cols)
                    for_right.append(error * left_cols)
                    at_rows.append(row)
                    at_cols.append(col)
                join = functools.partial(jnp.concatenate, axis=1)
                add(left_out, join(for_left), join(at_rows), a)
                add(right_out, join(for_right), join(at_cols), b)
                return 0

            lax.fori_loop(0, samples // ADD, batch, 0)

    for b in range(tile_cols):

        def over_rows(a, _, b=b):
            visit(a, b)
            return 0

        lax.fori_loop(0, tile_rows, over_rows, 0)


def on_device(
    coarse_left,
    coarse_right,
    stencil_left,
    weights_left,
    stencil_right,
    weights_right,
    tile_mask,
    sample_rows,
    sample_cols,
    sample_values,
):
    row, col = lax.axis_index("row"), lax.axis_index("col")
    left = lax.all_gather(with_edges(coarse_left, "row"), "col", axis=0, tiled=True)
    right = lax.all_gather(with_edges(coarse_right, "col"), "row", axis=0, tiled=True)
    left_rank, right_rank = coarse_left.shape[0], coarse_right.shape[0]
    place = jnp.stack(
        [
            col * left_rank,
            (col + 1) * left_rank,
            row * coarse_left.shape[1],
            row * right_rank,
            (row + 1) * right_rank,
            col * coarse_right.shape[1],
        ]
    ).astype(jnp.int32)
    rank = left.shape[0]
    tile_rows, tile_cols, _ = sample_rows.shape
    smem = pl.BlockSpec(memory_space=pltpu.SMEM)
    vmem = pl.BlockSpec(memory_space=pltpu.VMEM)
    table = (TILE // CHUNK * rank, 2 * CHUNK)
    left_out, right_out = pl.pallas_call(
        functools.partial(step, eta=4.0 * TILE / (SPT * TILES)),
        out_shape=(
            jax.ShapeDtypeStruct((rank, tile_rows * TILE), jnp.float32),
            jax.ShapeDtypeStruct((rank, tile_cols * TILE), jnp.float32),
        ),
        in_specs=[smem, smem] + [vmem] * 9,
        out_specs=(vmem, vmem),
        scratch_shapes=[
            pltpu.VMEM((tile_rows,) + table, jnp.bfloat16),
            pltpu.VMEM((tile_cols,) + table, jnp.bfloat16),
        ],
        compiler_params=pltpu.CompilerParams(vmem_limit_bytes=60 * 1024 * 1024),
    )(
        place,
        tile_mask,
        left,
        right,
        stencil_left.reshape(-1, 8, 128),
        weights_left,
        stencil_right.reshape(-1, 8, 128),
        weights_right,
        sample_rows,
        sample_cols,
        sample_values,
    )
    cols, rows = lax.axis_size("col"), lax.axis_size("row")
    left_parts = lax.all_to_all(
        left_out.reshape(cols, left_rank, -1), "col", 0, 0, tiled=False
    )
    right_parts = lax.all_to_all(
        right_out.reshape(rows, right_rank, -1), "row", 0, 0, tiled=False
    )
    return (jnp.sum(left_parts, axis=0), jnp.sum(right_parts, axis=0))


def solution(mesh):
    in_specs = (
        P("col", "row"),
        P("row", "col"),
        P("row"),
        P(None, "row"),
        P("col"),
        P(None, "col"),
        P("row", "col"),
        P("row", "col", None),
        P("row", "col", None),
        P("row", "col", None),
    )
    out_specs = (P("col", "row"), P("row", "col"))
    return jax.shard_map(
        on_device, mesh=mesh, in_specs=in_specs, out_specs=out_specs, check_vma=False
    )
```

```python
import functools

import jax
import jax.numpy as jnp
from jax import lax
from jax.experimental import pallas as pl
from jax.experimental.pallas import tpu as pltpu
from jax.sharding import PartitionSpec as P

TILES = 16
TILE = 4096
SPT = 2048
TAPS = 4
EDGE = 128
CHUNK = 256
READ = 1024
ADD = 1024


def split(values):
    high = values.astype(jnp.bfloat16)
    return high, (values - high.astype(jnp.float32)).astype(jnp.bfloat16)


def interpolate(padded, stencil, weights, table, out, me, offset, tile, own_rank):
    rank = padded.shape[0]
    own = lax.broadcasted_iota(jnp.int32, (rank, 128), 0) // own_rank == me

    def group(g, _):
        column = pl.multiple_of(tile * TILE + g * 1024, 1024)
        start = pl.multiple_of(tile * (TILE // 4) + g * 256, 256)
        base = stencil[tile * (TILE // 1024) + g] + (EDGE - 1 - offset - start)
        window = padded[:, pl.ds(start, 512)]
        for u in range(8):
            low = (EDGE - 2 + 32 * u) // 64 * 64
            if EDGE + 35 + 32 * u > low + 128:
                low += 64
            part = window[:, low : low + 128]
            total = None
            for t in range(TAPS):
                at = jnp.broadcast_to(base[u : u + 1, :] + (t - low), (rank, 128))
                taken = jnp.take_along_axis(part, at, axis=1, mode="promise_in_bounds")
                term = taken * weights[t : t + 1, pl.ds(column + 128 * u, 128)]
                total = term if total is None else total + term
            high, rest = split(total)
            to = pl.ds(pl.multiple_of((g * 4 + u // 2) * rank, rank), rank)
            lane = (u % 2) * 128
            table[tile, to, lane : lane + 128] = high
            table[tile, to, CHUNK + lane : CHUNK + lane + 128] = rest
            out[:, pl.ds(column + 128 * u, 128)] = jnp.where(own, total, 0.0)
        return 0

    lax.fori_loop(0, TILE // 1024, group, 0)


def one_hot(index):
    lanes = lax.broadcasted_iota(jnp.int32, (CHUNK, index.shape[1]), 0)
    return jnp.where(lanes == (index & (CHUNK - 1)), 1.0, 0.0).astype(jnp.bfloat16)


def read(table, index, rank):
    hot = one_hot(index)
    found = jnp.dot(
        table, jnp.concatenate([hot, hot], axis=0), preferred_element_type=jnp.float32
    )
    chunk = jnp.broadcast_to(index >> 8, (rank, index.shape[1]))
    taken = found[:rank]
    for c in range(1, found.shape[0] // rank):
        taken = jnp.where(chunk == c, found[c * rank : (c + 1) * rank], taken)
    return taken


def add(out, values, index, tile):
    rank = values.shape[0]
    hot = one_hot(index)
    chunk = jnp.broadcast_to(index >> 8, values.shape)
    high, rest = split(values)
    zero = jnp.zeros(values.shape, jnp.bfloat16)
    left = jnp.concatenate(
        [
            jnp.concatenate(
                [jnp.where(chunk == c, high, zero), jnp.where(chunk == c, rest, zero)], axis=1
            )
            for c in range(TILE // CHUNK)
        ],
        axis=0,
    )
    summed = lax.dot_general(
        left,
        jnp.concatenate([hot, hot], axis=1),
        (((1,), (1,)), ((), ())),
        preferred_element_type=jnp.float32,
    )
    for c in range(TILE // CHUNK):
        at = pl.ds(pl.multiple_of(tile * TILE + c * CHUNK, CHUNK), CHUNK)
        out[:, at] += summed[c * rank : (c + 1) * rank]


def pad(low, main, high, out):
    out[:, :EDGE] = low[...]
    out[:, EDGE : EDGE + main.shape[1]] = main[...]
    out[:, EDGE + main.shape[1] :] = high[...]


def step(
    place,
    mask,
    left_low,
    left,
    left_high,
    right_low,
    right,
    right_high,
    stencil_left,
    weights_left,
    stencil_right,
    weights_right,
    rows,
    cols,
    values,
    left_parts,
    right_parts,
    left_padded,
    right_padded,
    left_table,
    right_table,
    left_out,
    right_out,
    *,
    eta,
):
    rank = left.shape[0]
    tile_rows, tile_cols, samples = rows.shape
    me_row, me_col, left_offset, right_offset = (place[i] for i in range(4))
    left_rank, right_rank = left_parts.shape[2], right_parts.shape[1]
    pad(left_low, left, left_high, left_padded)
    pad(right_low, right, right_high, right_padded)
    for a in range(tile_rows):
        interpolate(
            left_padded, stencil_left, weights_left, left_table, left_out, me_col, left_offset, a, left_rank
        )
    for b in range(tile_cols):
        interpolate(
            right_padded, stencil_right, weights_right, right_table, right_out, me_row, right_offset, b, right_rank
        )

    def visit(a, b):
        @pl.when(mask[a, b] != 0)
        def _():
            scale = mask[a, b].astype(jnp.float32) * (-eta)

            def batch(i, _):
                for_left, for_right, at_rows, at_cols = [], [], [], []
                for j in range(ADD // READ):
                    at = pl.ds(pl.multiple_of(i * ADD + j * READ, READ), READ)
                    row = rows[a, b : b + 1, at]
                    col = cols[a, b : b + 1, at]
                    left_cols = read(left_table[a], row, rank)
                    right_cols = read(right_table[b], col, rank)
                    product = jnp.sum(left_cols * right_cols, axis=0, keepdims=True)
                    error = scale * (product - values[a, b : b + 1, at])
                    for_left.append(error * right_cols)
                    for_right.append(error * left_cols)
                    at_rows.append(row)
                    at_cols.append(col)
                join = functools.partial(jnp.concatenate, axis=1)
                add(left_out, join(for_left), join(at_rows), a)
                add(right_out, join(for_right), join(at_cols), b)
                return 0

            lax.fori_loop(0, samples // ADD, batch, 0)

    for b in range(tile_cols):

        def over_rows(a, _, b=b):
            visit(a, b)
            return 0

        lax.fori_loop(0, tile_rows, over_rows, 0)


    def left_group(i, _):
        at = pl.ds(pl.multiple_of(i * 512, 512), 512)
        part = left_out[:, at]
        for c in range(rank // left_rank):
            left_parts[(c % 2) ^ (me_col % 2), (c // 2) ^ (me_col // 2), :, at] = part[
                c * left_rank : (c + 1) * left_rank
            ]
        return 0

    def right_group(i, _):
        at = pl.ds(pl.multiple_of(i * 512, 512), 512)
        part = right_out[:, at]
        for r in range(rank // right_rank):
            right_parts[r ^ me_row, :, at] = part[r * right_rank : (r + 1) * right_rank]
        return 0

    lax.fori_loop(0, left_out.shape[1] // 512, left_group, 0)
    lax.fori_loop(0, right_out.shape[1] // 512, right_group, 0)


def swap(x, axis, distance):
    return lax.ppermute(x, axis, [(i, i ^ distance) for i in range(lax.axis_size(axis))])


def from_neighbours(x, axis):
    count = lax.axis_size(axis)
    forward = [(i, i + 1) for i in range(count - 1)]
    backward = [(target, source) for source, target in forward]
    low = lax.ppermute(x[:, x.shape[1] - EDGE :], axis, forward)
    high = lax.ppermute(x[:, :EDGE], axis, backward)
    return low, high


def put(buffer, x, index, axis=0):
    return lax.dynamic_update_index_in_dim(buffer, x, index, axis)


def gather(x, axis, me, count, unit):
    out = put(jnp.zeros((count,) + x.shape, x.dtype), x, me)
    for j in range(1, count):
        out = put(out, swap(x, axis, j * unit), me ^ j)
    return out


def halve(parts, axis, distances):
    parts = dict(enumerate(parts))
    for step in distances:
        kept = [j for j in parts if not j & step]
        sent = jnp.stack([parts[j ^ step] for j in kept])
        came = swap(sent, axis[0], step * axis[1])
        parts = {j: parts[j] + came[i] for i, j in enumerate(kept)}
    return parts


def on_device(
    coarse_left,
    coarse_right,
    stencil_left,
    weights_left,
    stencil_right,
    weights_right,
    tile_mask,
    sample_rows,
    sample_cols,
    sample_values,
):
    row, col = lax.axis_index("row"), lax.axis_index("col")
    rows, cols = lax.axis_size("row"), lax.axis_size("col")
    left_rank, left_width = coarse_left.shape
    right_rank, right_width = coarse_right.shape
    rank = left_rank * cols
    half = gather(coarse_left, "col", col // 2, cols // 2, 2)
    right = gather(coarse_right, "row", row, rows, 1).reshape(rank, right_width)
    right_low, right_high = from_neighbours(right, "col")
    other = swap(half, "col", 1)
    left = jnp.zeros((cols // 2, 2, left_rank, left_width), jnp.float32)
    left = put(put(left, half, col % 2, 1), other, 1 - col % 2, 1).reshape(rank, left_width)
    left_low, left_high = from_neighbours(left, "row")
    place = jnp.stack([row, col, row * left_width, col * right_width]).astype(jnp.int32)
    tile_rows, tile_cols, _ = sample_rows.shape
    smem = pl.BlockSpec(memory_space=pltpu.SMEM)
    vmem = pl.BlockSpec(memory_space=pltpu.VMEM)
    table = (TILE // CHUNK * rank, 2 * CHUNK)
    left_parts, right_parts = pl.pallas_call(
        functools.partial(step, eta=4.0 * TILE / (SPT * TILES)),
        out_shape=(
            jax.ShapeDtypeStruct((2, cols // 2, left_rank, tile_rows * TILE), jnp.float32),
            jax.ShapeDtypeStruct((rows, right_rank, tile_cols * TILE), jnp.float32),
        ),
        in_specs=[smem, smem] + [vmem] * 13,
        out_specs=(vmem, vmem),
        scratch_shapes=[
            pltpu.VMEM((rank, left_width + 2 * EDGE), jnp.float32),
            pltpu.VMEM((rank, right_width + 2 * EDGE), jnp.float32),
            pltpu.VMEM((tile_rows,) + table, jnp.bfloat16),
            pltpu.VMEM((tile_cols,) + table, jnp.bfloat16),
            pltpu.VMEM((rank, tile_rows * TILE), jnp.float32),
            pltpu.VMEM((rank, tile_cols * TILE), jnp.float32),
        ],
        compiler_params=pltpu.CompilerParams(vmem_limit_bytes=60 * 1024 * 1024),
    )(
        place,
        tile_mask,
        left_low,
        left,
        left_high,
        right_low,
        right,
        right_high,
        stencil_left.reshape(-1, 8, 128),
        weights_left,
        stencil_right.reshape(-1, 8, 128),
        weights_right,
        sample_rows,
        sample_cols,
        sample_values,
    )
    right_sum = halve(list(right_parts), ("row", 1), bits(rows))
    summed = left_parts[0] + swap(left_parts[1], "col", 1)
    left_sum = halve(list(summed), ("col", 2), bits(cols // 2))
    return (left_sum[0], right_sum[0])


def bits(count):
    out = []
    while count > 1:
        count //= 2
        out.append(count)
    return out[::-1]


def solution(mesh):
    in_specs = (
        P("col", "row"),
        P("row", "col"),
        P("row"),
        P(None, "row"),
        P("col"),
        P(None, "col"),
        P("row", "col"),
        P("row", "col", None),
        P("row", "col", None),
        P("row", "col", None),
    )
    out_specs = (P("col", "row"), P("row", "col"))
    return jax.shard_map(
        on_device, mesh=mesh, in_specs=in_specs, out_specs=out_specs, check_vma=False
    )
```

```python
import functools

import jax
import jax.numpy as jnp
from jax import lax
from jax.experimental import pallas as pl
from jax.experimental.pallas import tpu as pltpu
from jax.sharding import PartitionSpec as P


TILES = 16
TILE = 4096
SPT = 2048
TAPS = 4
EDGE = 128
CHUNK = 256
BATCH = 1024


def split(values):
    high = values.astype(jnp.bfloat16)
    return high, (values - high.astype(jnp.float32)).astype(jnp.bfloat16)


def interpolate(padded, stencil, weights, keep, out, me, offset, tile, own_rank):
    rank = padded.shape[0]
    own = lax.broadcasted_iota(jnp.int32, (rank, 128), 0) // own_rank == me

    def group(g, _):
        column = pl.multiple_of(tile * TILE + g * 1024, 1024)
        start = pl.multiple_of(tile * (TILE // 4) + g * 256, 256)
        base = stencil[tile * (TILE // 1024) + g] + (EDGE - 1 - offset - start)
        window = padded[:, pl.ds(start, 512)]
        for u in range(8):
            low = (EDGE - 2 + 32 * u) // 64 * 64
            if EDGE + 35 + 32 * u > low + 128:
                low += 64
            part = window[:, low : low + 128]
            total = [None] * (rank // 8)
            for t in range(TAPS):
                at = jnp.broadcast_to(base[u : u + 1, :] + (t - low), (8, 128))
                weight = jnp.broadcast_to(weights[t : t + 1, pl.ds(column + 128 * u, 128)], (8, 128))
                for k in range(rank // 8):
                    taken = jnp.take_along_axis(
                        part[8 * k : 8 * k + 8], at, axis=1, mode="promise_in_bounds"
                    )
                    term = taken * weight
                    total[k] = term if total[k] is None else total[k] + term
            total = jnp.concatenate(total, axis=0)
            keep(g, u, total)
            out[:, pl.ds(column + 128 * u, 128)] = jnp.where(own, total, 0.0)
        return 0

    lax.fori_loop(0, TILE // 1024, group, 0)


def keep_split(table, tile):
    def keep(g, u, total):
        rank = total.shape[0]
        high, rest = split(total)
        to = pl.ds(pl.multiple_of((g * 4 + u // 2) * rank, rank), rank)
        lane = (u % 2) * 128
        table[tile, to, lane : lane + 128] = high
        table[tile, to, CHUNK + lane : CHUNK + lane + 128] = rest

    return keep


def keep_whole(table, tile):
    def keep(g, u, total):
        table[tile, :, pl.ds(pl.multiple_of(g * 1024 + u * 128, 128), 128)] = total

    return keep


def one_hot(index):
    lanes = lax.broadcasted_iota(jnp.int32, (CHUNK, index.shape[1]), 0)
    return jnp.where(lanes == (index & (CHUNK - 1)), 1.0, 0.0).astype(jnp.bfloat16)


def read(table, index, rank):
    hot = one_hot(index)
    found = jnp.dot(
        table, jnp.concatenate([hot, hot], axis=0), preferred_element_type=jnp.float32
    )
    chunk = jnp.broadcast_to(index >> 8, (rank, index.shape[1]))
    taken = found[:rank]
    for c in range(1, found.shape[0] // rank):
        taken = jnp.where(chunk == c, found[c * rank : (c + 1) * rank], taken)
    return taken


def read_lanes(table, index):
    rank, width = table.shape
    found = []
    for s in range(index.shape[1] // 128):
        at = jnp.broadcast_to(index[:, s * 128 : (s + 1) * 128], (8, 128))
        lane, chunk = at & 127, at >> 7
        taken = [None] * (rank // 8)
        for c in range(width // 128):
            for k in range(rank // 8):
                here = jnp.take_along_axis(
                    table[8 * k : 8 * k + 8, c * 128 : (c + 1) * 128],
                    lane,
                    axis=1,
                    mode="promise_in_bounds",
                )
                taken[k] = here if c == 0 else jnp.where(chunk == c, here, taken[k])
        found.append(jnp.concatenate(taken, axis=0))
    return jnp.concatenate(found, axis=1)


def add(out, values, index, tile):
    rank = values.shape[0]
    hot = one_hot(index)
    chunk = jnp.broadcast_to(index >> 8, values.shape)
    high, rest = split(values)
    zero = jnp.zeros(values.shape, jnp.bfloat16)
    left = jnp.concatenate(
        [
            jnp.concatenate(
                [jnp.where(chunk == c, high, zero), jnp.where(chunk == c, rest, zero)], axis=1
            )
            for c in range(TILE // CHUNK)
        ],
        axis=0,
    )
    summed = lax.dot_general(
        left,
        jnp.concatenate([hot, hot], axis=1),
        (((1,), (1,)), ((), ())),
        preferred_element_type=jnp.float32,
    )
    for c in range(TILE // CHUNK):
        at = pl.ds(pl.multiple_of(tile * TILE + c * CHUNK, CHUNK), CHUNK)
        out[:, at] += summed[c * rank : (c + 1) * rank]


def pad(low, main, high, out):
    out[:, :EDGE] = low[...]
    out[:, EDGE : EDGE + main.shape[1]] = main[...]
    out[:, EDGE + main.shape[1] :] = high[...]


def step(
    mask,
    left_low,
    left,
    left_high,
    right_low,
    right,
    right_high,
    stencil_left,
    weights_left,
    stencil_right,
    weights_right,
    rows,
    cols,
    values,
    left_parts,
    right_parts,
    left_padded,
    right_padded,
    left_table,
    right_table,
    left_out,
    right_out,
    even,
    odd,
    live,
    *,
    eta,
):
    rank = left.shape[0]
    tile_rows, tile_cols, samples = rows.shape
    me_row, me_col = lax.axis_index("row"), lax.axis_index("col")
    left_rank, right_rank = left_parts.shape[3], right_parts.shape[2]
    pad(left_low, left, left_high, left_padded)
    pad(right_low, right, right_high, right_padded)
    for a in range(tile_rows):
        interpolate(
            left_padded,
            stencil_left,
            weights_left,
            keep_split(left_table, a),
            left_out,
            me_col,
            me_row * left.shape[1],
            a,
            left_rank,
        )
    for b in range(tile_cols):
        interpolate(
            right_padded,
            stencil_right,
            weights_right,
            keep_whole(right_table, b),
            right_out,
            me_row,
            me_col * right.shape[1],
            b,
            right_rank,
        )

    count = jnp.int32(0)
    for tile in range(tile_rows * tile_cols):
        live[count] = tile
        count += (mask[tile // tile_cols, tile % tile_cols] != 0).astype(jnp.int32)
    held = (even, odd)
    batches = samples // BATCH
    even[...] = jnp.zeros_like(even)
    odd[...] = jnp.zeros_like(odd)

    def listed(array, tile, i):
        part = array[tile // tile_cols, :, i * BATCH : (i + 1) * BATCH]
        row = part[:1]
        for b in range(1, tile_cols):
            row = jnp.where(tile % tile_cols == b, part[b : b + 1], row)
        return row

    def errors(tile, i):
        a, b = tile // tile_cols, tile % tile_cols
        scale = mask[a, b].astype(jnp.float32) * (-eta)
        left_cols = read(left_table[a], listed(rows, tile, i), rank)
        right_cols = read_lanes(right_table.at[b], listed(cols, tile, i))
        product = jnp.sum(left_cols * right_cols, axis=0, keepdims=True)
        error = scale * (product - listed(values, tile, i))
        held[i % 2][0] = error * right_cols
        held[i % 2][1] = error * left_cols

    def adds(tile, i):
        add(left_out, held[i % 2][0], listed(rows, tile, i), tile // tile_cols)
        add(right_out, held[i % 2][1], listed(cols, tile, i), tile % tile_cols)

    def visit(n, _):
        tile, before = live[n], live[jnp.maximum(n - 1, 0)]
        for i in range(batches):
            if i:
                adds(tile, i - 1)
            else:
                adds(before, batches - 1)
            errors(tile, i)
        return 0

    lax.fori_loop(0, count, visit, 0)

    @pl.when(count > 0)
    def _():
        adds(live[count - 1], batches - 1)

    def left_group(i, _):
        half = left_parts.shape[4]
        for h in range(2):
            at = pl.multiple_of(i * 512, 512)
            part = left_out[:, pl.ds(h * half + at, 512)]
            for c in range(rank // left_rank):
                left_parts[h, (c % 2) ^ (me_col % 2), (c // 2) ^ (me_col // 2), :, pl.ds(at, 512)] = (
                    part[c * left_rank : (c + 1) * left_rank]
                )
        return 0

    def right_group(i, _):
        half = right_parts.shape[3]
        for h in range(2):
            at = pl.multiple_of(i * 512, 512)
            part = right_out[:, pl.ds(h * half + at, 512)]
            for r in range(rank // right_rank):
                right_parts[h, r ^ me_row, :, pl.ds(at, 512)] = part[
                    r * right_rank : (r + 1) * right_rank
                ]
        return 0

    lax.fori_loop(0, left_parts.shape[4] // 512, left_group, 0)
    lax.fori_loop(0, right_parts.shape[3] // 512, right_group, 0)


def swap(x, axis, distance):
    return lax.ppermute(x, axis, [(i, i ^ distance) for i in range(lax.axis_size(axis))])


def from_neighbours(x, axis):
    count = lax.axis_size(axis)
    forward = [(i, i + 1) for i in range(count - 1)]
    backward = [(target, source) for source, target in forward]
    low = lax.ppermute(x[:, x.shape[1] - EDGE :], axis, forward)
    high = lax.ppermute(x[:, :EDGE], axis, backward)
    return low, high


def put(buffer, x, index, axis=0):
    return lax.dynamic_update_index_in_dim(buffer, x, index, axis)


def gather(x, axis, me, count, unit):
    out = put(jnp.zeros((count,) + x.shape, x.dtype), x, me)
    for j in range(1, count):
        out = put(out, swap(x, axis, j * unit), me ^ j)
    return out


def halve(parts, axis, distances):
    parts = {j: parts[j] for j in range(parts.shape[0])}
    for step in distances:
        kept = [j for j in parts if not j & step]
        sent = jnp.stack([parts[j ^ step] for j in kept])
        came = swap(sent, axis[0], step * axis[1])
        parts = {j: parts[j] + came[i] for i, j in enumerate(kept)}
    return parts[0]


def on_device(
    coarse_left,
    coarse_right,
    stencil_left,
    weights_left,
    stencil_right,
    weights_right,
    tile_mask,
    sample_rows,
    sample_cols,
    sample_values,
):
    row, col = lax.axis_index("row"), lax.axis_index("col")
    rows, cols = lax.axis_size("row"), lax.axis_size("col")
    left_rank, left_width = coarse_left.shape
    right_rank, right_width = coarse_right.shape
    rank = left_rank * cols
    half = gather(coarse_left, "col", col // 2, cols // 2, 2)
    right = gather(coarse_right, "row", row, rows, 1).reshape(rank, right_width)
    right_low, right_high = from_neighbours(right, "col")
    other = swap(half, "col", 1)
    left = jnp.zeros((cols // 2, 2, left_rank, left_width), jnp.float32)
    left = put(put(left, half, col % 2, 1), other, 1 - col % 2, 1).reshape(rank, left_width)
    left_low, left_high = from_neighbours(left, "row")
    tile_rows, tile_cols, _ = sample_rows.shape
    smem = pl.BlockSpec(memory_space=pltpu.SMEM)
    vmem = pl.BlockSpec(memory_space=pltpu.VMEM)
    left_parts, right_parts = pl.pallas_call(
        functools.partial(step, eta=4.0 * TILE / (SPT * TILES)),
        out_shape=(
            jax.ShapeDtypeStruct((2, 2, cols // 2, left_rank, tile_rows * TILE // 2), jnp.float32),
            jax.ShapeDtypeStruct((2, rows, right_rank, tile_cols * TILE // 2), jnp.float32),
        ),
        in_specs=[smem] + [vmem] * 13,
        out_specs=(vmem, vmem),
        scratch_shapes=[
            pltpu.VMEM((rank, left_width + 2 * EDGE), jnp.float32),
            pltpu.VMEM((rank, right_width + 2 * EDGE), jnp.float32),
            pltpu.VMEM((tile_rows, TILE // CHUNK * rank, 2 * CHUNK), jnp.bfloat16),
            pltpu.VMEM((tile_cols, rank, TILE), jnp.float32),
            pltpu.VMEM((rank, tile_rows * TILE), jnp.float32),
            pltpu.VMEM((rank, tile_cols * TILE), jnp.float32),
            pltpu.VMEM((2, rank, BATCH), jnp.float32),
            pltpu.VMEM((2, rank, BATCH), jnp.float32),
            pltpu.SMEM((tile_rows * tile_cols + 1,), jnp.int32),
        ],
        compiler_params=pltpu.CompilerParams(vmem_limit_bytes=60 * 1024 * 1024),
    )(
        tile_mask,
        left_low,
        left,
        left_high,
        right_low,
        right,
        right_high,
        stencil_left.reshape(-1, 8, 128),
        weights_left,
        stencil_right.reshape(-1, 8, 128),
        weights_right,
        sample_rows,
        sample_cols,
        sample_values,
    )
    came = swap(left_parts[:, 1], "col", 1)
    left_added, right_parts = lax.optimization_barrier((left_parts[:, 0] + came, right_parts))
    left_sums, right_sums = [], []
    for h in range(2):
        turned = slice(None, None, 1 - 2 * h)
        left_sums.append(halve(left_added[h], ("col", 2), bits(cols // 2)[turned]))
        right_sums.append(halve(right_parts[h], ("row", 1), bits(rows)[turned]))
    return (jnp.concatenate(left_sums, axis=1), jnp.concatenate(right_sums, axis=1))


def bits(count):
    out = []
    while count > 1:
        count //= 2
        out.append(count)
    return out[::-1]


def solution(mesh):
    in_specs = (
        P("col", "row"),
        P("row", "col"),
        P("row"),
        P(None, "row"),
        P("col"),
        P(None, "col"),
        P("row", "col"),
        P("row", "col", None),
        P("row", "col", None),
        P("row", "col", None),
    )
    out_specs = (P("col", "row"), P("row", "col"))

    return jax.shard_map(
        on_device, mesh=mesh, in_specs=in_specs, out_specs=out_specs, check_vma=False
    )
```

```python
import functools

import jax
import jax.numpy as jnp
from jax import lax
from jax.experimental import pallas as pl
from jax.experimental.pallas import tpu as pltpu
from jax.sharding import PartitionSpec as P


TILES = 16
TILE = 4096
SPT = 2048
TAPS = 4
EDGE = 128
CHUNK = 256
BATCH = 1024


def split(values):
    high = values.astype(jnp.bfloat16)
    return high, (values - high.astype(jnp.float32)).astype(jnp.bfloat16)


def interpolate(padded, stencil, weights, keep, out, me, offset, tile, own_rank):
    rank = padded.shape[0]
    own = lax.broadcasted_iota(jnp.int32, (rank, 128), 0) // own_rank == me

    def group(g, _):
        column = pl.multiple_of(tile * TILE + g * 1024, 1024)
        start = pl.multiple_of(tile * (TILE // 4) + g * 256, 256)
        base = stencil[tile * (TILE // 1024) + g] + (EDGE - 1 - offset - start)
        window = padded[:, pl.ds(start, 512)]
        for u in range(8):
            low = (EDGE - 2 + 32 * u) // 64 * 64
            if EDGE + 35 + 32 * u > low + 128:
                low += 64
            part = window[:, low : low + 128]
            total = [None] * (rank // 8)
            for t in range(TAPS):
                at = jnp.broadcast_to(base[u : u + 1, :] + (t - low), (8, 128))
                weight = jnp.broadcast_to(weights[t : t + 1, pl.ds(column + 128 * u, 128)], (8, 128))
                for k in range(rank // 8):
                    taken = jnp.take_along_axis(
                        part[8 * k : 8 * k + 8], at, axis=1, mode="promise_in_bounds"
                    )
                    term = taken * weight
                    total[k] = term if total[k] is None else total[k] + term
            total = jnp.concatenate(total, axis=0)
            keep(g, u, total)
            out[:, pl.ds(column + 128 * u, 128)] = jnp.where(own, total, 0.0)
        return 0

    lax.fori_loop(0, TILE // 1024, group, 0)


def keep_split(table, tile):
    def keep(g, u, total):
        rank = total.shape[0]
        high, rest = split(total)
        to = pl.ds(pl.multiple_of((g * 4 + u // 2) * rank, rank), rank)
        lane = (u % 2) * 128
        table[tile, to, lane : lane + 128] = high
        table[tile, to, CHUNK + lane : CHUNK + lane + 128] = rest

    return keep


def keep_whole(table, tile):
    def keep(g, u, total):
        table[tile, :, pl.ds(pl.multiple_of(g * 1024 + u * 128, 128), 128)] = total

    return keep


def one_hot(index):
    lanes = lax.broadcasted_iota(jnp.int32, (CHUNK, index.shape[1]), 0)
    return jnp.where(lanes == (index & (CHUNK - 1)), 1.0, 0.0).astype(jnp.bfloat16)


def read(table, index, rank):
    hot = one_hot(index)
    found = jnp.dot(
        table, jnp.concatenate([hot, hot], axis=0), preferred_element_type=jnp.float32
    )
    chunk = jnp.broadcast_to(index >> 8, (rank, index.shape[1]))
    taken = found[:rank]
    for c in range(1, found.shape[0] // rank):
        taken = jnp.where(chunk == c, found[c * rank : (c + 1) * rank], taken)
    return taken


def read_lanes(table, index):
    rank, width = table.shape
    found = []
    for s in range(index.shape[1] // 128):
        at = jnp.broadcast_to(index[:, s * 128 : (s + 1) * 128], (8, 128))
        lane, chunk = at & 127, at >> 7
        taken = [None] * (rank // 8)
        for c in range(width // 128):
            for k in range(rank // 8):
                here = jnp.take_along_axis(
                    table[8 * k : 8 * k + 8, c * 128 : (c + 1) * 128],
                    lane,
                    axis=1,
                    mode="promise_in_bounds",
                )
                taken[k] = here if c == 0 else jnp.where(chunk == c, here, taken[k])
        found.append(jnp.concatenate(taken, axis=0))
    return jnp.concatenate(found, axis=1)


def add(out, values, index, tile):
    rank = values.shape[0]
    hot = one_hot(index)
    chunk = jnp.broadcast_to(index >> 8, values.shape)
    high, rest = split(values)
    zero = jnp.zeros(values.shape, jnp.bfloat16)
    left = jnp.concatenate(
        [
            jnp.concatenate(
                [jnp.where(chunk == c, high, zero), jnp.where(chunk == c, rest, zero)], axis=1
            )
            for c in range(TILE // CHUNK)
        ],
        axis=0,
    )
    summed = lax.dot_general(
        left,
        jnp.concatenate([hot, hot], axis=1),
        (((1,), (1,)), ((), ())),
        preferred_element_type=jnp.float32,
    )
    for c in range(TILE // CHUNK):
        at = pl.ds(pl.multiple_of(tile * TILE + c * CHUNK, CHUNK), CHUNK)
        out[:, at] += summed[c * rank : (c + 1) * rank]


def pad(low, main, high, out):
    out[:, :EDGE] = low[...]
    out[:, EDGE : EDGE + main.shape[1]] = main[...]
    out[:, EDGE + main.shape[1] :] = high[...]


def step(
    mask,
    left,
    right_low,
    right,
    right_high,
    stencil_left,
    weights_left,
    stencil_right,
    weights_right,
    rows,
    cols,
    values,
    left_kept,
    left_sent,
    right_parts,
    right_padded,
    left_table,
    right_table,
    left_out,
    right_out,
    even,
    odd,
    live,
    *,
    eta,
):
    rank = left.shape[0]
    tile_rows, tile_cols, samples = rows.shape
    me_row, me_col = lax.axis_index("row"), lax.axis_index("col")
    left_rank, right_rank = left_kept.shape[2], right_parts.shape[1]
    pad(right_low, right, right_high, right_padded)
    for a in range(tile_rows):
        interpolate(
            left,
            stencil_left,
            weights_left,
            keep_split(left_table, a),
            left_out,
            me_col,
            me_row * (left.shape[1] - 2 * EDGE),
            a,
            left_rank,
        )
    for b in range(tile_cols):
        interpolate(
            right_padded,
            stencil_right,
            weights_right,
            keep_whole(right_table, b),
            right_out,
            me_row,
            me_col * right.shape[1],
            b,
            right_rank,
        )

    count = jnp.int32(0)
    for tile in range(tile_rows * tile_cols):
        live[count] = tile
        count += (mask[tile // tile_cols, tile % tile_cols] != 0).astype(jnp.int32)
    held = (even, odd)
    batches = samples // BATCH
    even[...] = jnp.zeros_like(even)
    odd[...] = jnp.zeros_like(odd)

    def listed(array, tile, i):
        part = array[tile // tile_cols, :, i * BATCH : (i + 1) * BATCH]
        row = part[:1]
        for b in range(1, tile_cols):
            row = jnp.where(tile % tile_cols == b, part[b : b + 1], row)
        return row

    def errors(tile, i):
        a, b = tile // tile_cols, tile % tile_cols
        scale = mask[a, b].astype(jnp.float32) * (-eta)
        left_cols = read(left_table[a], listed(rows, tile, i), rank)
        right_cols = read_lanes(right_table.at[b], listed(cols, tile, i))
        product = jnp.sum(left_cols * right_cols, axis=0, keepdims=True)
        error = scale * (product - listed(values, tile, i))
        held[i % 2][0] = error * right_cols
        held[i % 2][1] = error * left_cols

    def adds(tile, i):
        add(left_out, held[i % 2][0], listed(rows, tile, i), tile // tile_cols)
        add(right_out, held[i % 2][1], listed(cols, tile, i), tile % tile_cols)

    def visit(n, _):
        tile, before = live[n], live[jnp.maximum(n - 1, 0)]
        for i in range(batches):
            if i:
                adds(tile, i - 1)
            else:
                adds(before, batches - 1)
            errors(tile, i)
        return 0

    lax.fori_loop(0, count, visit, 0)

    @pl.when(count > 0)
    def _():
        adds(live[count - 1], batches - 1)

    def left_group(i, _):
        half = left_kept.shape[3]
        for h in range(2):
            at = pl.multiple_of(i * 512, 512)
            part = left_out[:, pl.ds(h * half + at, 512)]
            for g in range(rank // left_rank // 2):
                low = part[2 * g * left_rank : (2 * g + 1) * left_rank]
                high = part[(2 * g + 1) * left_rank : (2 * g + 2) * left_rank]
                to = (h, g ^ (me_col // 2), slice(None), pl.ds(at, 512))
                left_kept[to] = jnp.where(me_col % 2 == 0, low, high)
                left_sent[to] = jnp.where(me_col % 2 == 0, high, low)
        return 0

    def right_group(i, _):
        at = pl.ds(pl.multiple_of(i * 512, 512), 512)
        part = right_out[:, at]
        for r in range(rank // right_rank):
            right_parts[r ^ me_row, :, at] = part[r * right_rank : (r + 1) * right_rank]
        return 0

    lax.fori_loop(0, left_kept.shape[3] // 512, left_group, 0)
    lax.fori_loop(0, right_parts.shape[2] // 512, right_group, 0)


def swap(x, axis, distance):
    return lax.ppermute(x, axis, [(i, i ^ distance) for i in range(lax.axis_size(axis))])


def from_neighbours(x, axis):
    count = lax.axis_size(axis)
    forward = [(i, i + 1) for i in range(count - 1)]
    backward = [(target, source) for source, target in forward]
    low = lax.ppermute(x[:, x.shape[1] - EDGE :], axis, forward)
    high = lax.ppermute(x[:, :EDGE], axis, backward)
    return low, high


def put(buffer, x, index, axis=0):
    return lax.dynamic_update_index_in_dim(buffer, x, index, axis)


def gather(x, axis, me, count, unit):
    out = put(jnp.zeros((count,) + x.shape, x.dtype), x, me)
    for j in range(1, count):
        out = put(out, swap(x, axis, j * unit), me ^ j)
    return out


def halve(parts, axis, step):
    kept = [j for j in parts if not j & step]
    sent = jnp.stack([parts[j ^ step] for j in kept])
    came = swap(sent, axis[0], step * axis[1])
    return {j: parts[j] + came[i] for i, j in enumerate(kept)}


def on_device(
    coarse_left,
    coarse_right,
    stencil_left,
    weights_left,
    stencil_right,
    weights_right,
    tile_mask,
    sample_rows,
    sample_cols,
    sample_values,
):
    row, col = lax.axis_index("row"), lax.axis_index("col")
    rows, cols = lax.axis_size("row"), lax.axis_size("col")
    left_rank, left_width = coarse_left.shape
    right_rank, right_width = coarse_right.shape
    rank = left_rank * cols
    edges = jnp.concatenate([coarse_left[:, :EDGE], coarse_left[:, left_width - EDGE :]], axis=1)
    packed = jnp.concatenate([coarse_right, edges.reshape(right_rank, -1)], axis=1)
    packed = gather(packed, "row", row, rows, 1)
    edges = packed[:, :, right_width:].reshape(rows, left_rank, 2, EDGE)
    low = jnp.where(row > 0, edges[jnp.maximum(row - 1, 0), :, 1], 0.0)
    high = jnp.where(row < rows - 1, edges[jnp.minimum(row + 1, rows - 1), :, 0], 0.0)
    own = jnp.concatenate([low, coarse_left, high], axis=1)
    half = gather(own, "col", col // 2, cols // 2, 2)
    right = packed[:, :, :right_width].reshape(rank, right_width)
    right_low, right_high = from_neighbours(right, "col")
    other = swap(half, "col", 1)
    left = jnp.zeros((cols // 2, 2) + own.shape, jnp.float32)
    left = put(put(left, half, col % 2, 1), other, 1 - col % 2, 1).reshape(rank, -1)
    tile_rows, tile_cols, _ = sample_rows.shape
    smem = pl.BlockSpec(memory_space=pltpu.SMEM)
    vmem = pl.BlockSpec(memory_space=pltpu.VMEM)
    left_kept, left_sent, right_parts = pl.pallas_call(
        functools.partial(step, eta=4.0 * TILE / (SPT * TILES)),
        out_shape=(
            jax.ShapeDtypeStruct((2, cols // 2, left_rank, tile_rows * TILE // 2), jnp.float32),
            jax.ShapeDtypeStruct((2, cols // 2, left_rank, tile_rows * TILE // 2), jnp.float32),
            jax.ShapeDtypeStruct((rows, right_rank, tile_cols * TILE), jnp.float32),
        ),
        in_specs=[smem] + [vmem] * 11,
        out_specs=(vmem, vmem, vmem),
        scratch_shapes=[
            pltpu.VMEM((rank, right_width + 2 * EDGE), jnp.float32),
            pltpu.VMEM((tile_rows, TILE // CHUNK * rank, 2 * CHUNK), jnp.bfloat16),
            pltpu.VMEM((tile_cols, rank, TILE), jnp.float32),
            pltpu.VMEM((rank, tile_rows * TILE), jnp.float32),
            pltpu.VMEM((rank, tile_cols * TILE), jnp.float32),
            pltpu.VMEM((2, rank, BATCH), jnp.float32),
            pltpu.VMEM((2, rank, BATCH), jnp.float32),
            pltpu.SMEM((tile_rows * tile_cols + 1,), jnp.int32),
        ],
        compiler_params=pltpu.CompilerParams(vmem_limit_bytes=60 * 1024 * 1024),
    )(
        tile_mask,
        left,
        right_low,
        right,
        right_high,
        stencil_left.reshape(-1, 8, 128),
        weights_left,
        stencil_right.reshape(-1, 8, 128),
        weights_right,
        sample_rows,
        sample_cols,
        sample_values,
    )
    left_added, right_parts = lax.optimization_barrier(
        (left_kept + swap(left_sent, "col", 1), right_parts)
    )
    sums = [
        [left_added[0], ("col", 2), bits(cols // 2)],
        [left_added[1], ("col", 2), bits(cols // 2)[::-1]],
        [right_parts, ("row", 1), bits(rows)],
    ]
    held = [{j: parts[j] for j in range(parts.shape[0])} for parts, _, _ in sums]
    for turn in range(max(len(steps) for _, _, steps in sums)):
        if turn:
            held = lax.optimization_barrier(held)
        for i, (_, axis, steps) in enumerate(sums):
            if turn < len(steps):
                held[i] = halve(held[i], axis, steps[turn])
    left_low, left_high, right = (parts[0] for parts in held)
    return (jnp.concatenate([left_low, left_high], axis=1), right)


def bits(count):
    out = []
    while count > 1:
        count //= 2
        out.append(count)
    return out[::-1]


def solution(mesh):
    in_specs = (
        P("col", "row"),
        P("row", "col"),
        P("row"),
        P(None, "row"),
        P("col"),
        P(None, "col"),
        P("row", "col"),
        P("row", "col", None),
        P("row", "col", None),
        P("row", "col", None),
    )
    out_specs = (P("col", "row"), P("row", "col"))

    return jax.shard_map(
        on_device, mesh=mesh, in_specs=in_specs, out_specs=out_specs, check_vma=False
    )
```
